32 devices in a mesh: dp: 4 (over z), tensor: 8 (over y, x, core).
Axes of the slice: x: 2, y: 2, z: 4, core: 2. Of those that a mesh axis runs over, the one named last changes fastest.
Arguments:
- residual: float32 [8192, 4096], P(('dp', 'tensor')), may hold values from -6 to 6
- cotangent: bfloat16 [8192, 4096], P(('dp', 'tensor')), may hold values from -6 to 6
- segments: int32 [8, 1024], P('dp'), may hold values from 0 to 7, never falling along the last dimension, each value on 1 to 800 neighbouring positions
- in_proj: bfloat16 [4096, 32, 384], P('dp', 'tensor'), as said below
- qv_bias: bfloat16 [32, 256], P('tensor', 'dp'), may hold values from -1.5 to 1.5
- out_proj: bfloat16 [4096, 4096], P('tensor', 'dp'), may hold values from -0.25 to 0.25
- up_proj: bfloat16 [4096, 16384], P('dp', 'tensor'), may hold values from -0.09375 to 0.09375
- up_bias: bfloat16 [16384], P(('tensor', 'dp')), may hold values from -3 to 3
- down_proj: bfloat16 [16384, 4096], P('tensor', 'dp'), may hold values from -0.046875 to 0.046875
- norm_params: bfloat16 [4, 4096], replicated, may hold values from 0.099609375 to 1.8984375
- out_biases: bfloat16 [2, 4096], replicated, may hold values from -3 to 3
- first_in_proj: float32 [4096, 32, 384], P('dp', 'tensor'), may hold values from -16 to 16
- first_qv_bias: float32 [32, 256], P('tensor', 'dp'), may hold values from -16 to 16
- first_out_proj: float32 [4096, 4096], P('tensor', 'dp'), may hold values from -16 to 16
- first_up_proj: float32 [4096, 16384], P('dp', 'tensor'), may hold values from -16 to 16
- first_up_bias: float32 [16384], P(('tensor', 'dp')), may hold values from -16 to 16
- first_down_proj: float32 [16384, 4096], P('tensor', 'dp'), may hold values from -16 to 16
- first_norm_params: float32 [4, 4096], replicated, may hold values from -16 to 16
- first_out_biases: float32 [2, 4096], replicated, may hold values from -16 to 16
- second_in_proj: float32 [4096, 32, 384], P('dp', 'tensor'), may hold values from 1 to 100
- second_qv_bias: float32 [32, 256], P('tensor', 'dp'), may hold values from 1 to 100
- second_out_proj: float32 [4096, 4096], P('tensor', 'dp'), may hold values from 1 to 100
- second_up_proj: float32 [4096, 16384], P('dp', 'tensor'), may hold values from 1 to 100
- second_up_bias: float32 [16384], P(('tensor', 'dp')), may hold values from 1 to 100
- second_down_proj: float32 [16384, 4096], P('tensor', 'dp'), may hold values from 1 to 100
- second_norm_params: float32 [4, 4096], replicated, may hold values from 1 to 100
- second_out_biases: float32 [2, 4096], replicated, may hold values from 1 to 100
Outputs:
- output: float32 [8192, 4096], P(('dp', 'tensor'))
- grad_residual: float32 [8192, 4096], P(('dp', 'tensor'))
- grad_in_proj: float32 [4096, 32, 384], P('dp', 'tensor')
- new_in_proj: float32 [4096, 32, 384], P('dp', 'tensor')
- new_first_in_proj: float32 [4096, 32, 384], P('dp', 'tensor')
- new_second_in_proj: float32 [4096, 32, 384], P('dp', 'tensor')
- grad_qv_bias: float32 [32, 256], P('tensor', 'dp')
- new_qv_bias: float32 [32, 256], P('tensor', 'dp')
- new_first_qv_bias: float32 [32, 256], P('tensor', 'dp')
- new_second_qv_bias: float32 [32, 256], P('tensor', 'dp')
- grad_out_proj: float32 [4096, 4096], P('tensor', 'dp')
- new_out_proj: float32 [4096, 4096], P('tensor', 'dp')
- new_first_out_proj: float32 [4096, 4096], P('tensor', 'dp')
- new_second_out_proj: float32 [4096, 4096], P('tensor', 'dp')
- grad_up_proj: float32 [4096, 16384], P('dp', 'tensor')
- new_up_proj: float32 [4096, 16384], P('dp', 'tensor')
- new_first_up_proj: float32 [4096, 16384], P('dp', 'tensor')
- new_second_up_proj: float32 [4096, 16384], P('dp', 'tensor')
- grad_up_bias: float32 [16384], P(('tensor', 'dp'))
- new_up_bias: float32 [16384], P(('tensor', 'dp'))
- new_first_up_bias: float32 [16384], P(('tensor', 'dp'))
- new_second_up_bias: float32 [16384], P(('tensor', 'dp'))
- grad_down_proj: float32 [16384, 4096], P('tensor', 'dp')
- new_down_proj: float32 [16384, 4096], P('tensor', 'dp')
- new_first_down_proj: float32 [16384, 4096], P('tensor', 'dp')
- new_second_down_proj: float32 [16384, 4096], P('tensor', 'dp')
- grad_norm_params: float32 [4, 4096], replicated
- new_norm_params: float32 [4, 4096], replicated
- new_first_norm_params: float32 [4, 4096], replicated
- new_second_norm_params: float32 [4, 4096], replicated
- grad_out_biases: float32 [2, 4096], replicated
- new_out_biases: float32 [2, 4096], replicated
- new_first_out_biases: float32 [2, 4096], replicated
- new_second_out_biases: float32 [2, 4096], replicated
The draws below stay inside these ranges and needn't reach their ends.
Inputs may be any that keep to these rules, and one draw needn't show every extreme that they name: `segments`: segment numbers never fall along a sequence; every segment holds 1 to 800 tokens, and some segment exactly 800. `in_proj`: entries of magnitude at most 36 times the inverse root of 4096.
All inputs are finite; a program needn't handle non-finite values.
Results may differ from the reference program's by a relative error of at most 0.0095.
The reference program's roundings to bfloat16 on the way count: a program that leaves them out, or rounds other values in their place, can miss the bound.
Values may be sent and summed in bfloat16 or wider, within the bound.
A program may use at most 640 MiB of HBM per device.

```python
import math
import jax
import jax.numpy as jnp
import numpy as np
from jax import lax

D = 4096
H = 32
HD = 128
ROT = 32
FF = 16384
SEQ_LEN = 1024
STEP = 8
DOCS = 8
DOC_MOST = 800
SEQS = 8
TOKENS = 8192


def draw_in_proj(key, part):
    base = jnp.clip(jax.random.normal(key, (D, H, 3 * HD), jnp.float32), -6.0, 6.0) * (1.0 / math.sqrt(D))
    return base.astype(jnp.bfloat16)


def level_of(key, extent, pieces, smallest, high):
    gain = 1.0
    for axis_at, blocks in pieces:
        draws = jax.random.uniform(jax.random.fold_in(jax.random.fold_in(key, 6), axis_at), (blocks,), jnp.float32, smallest / len(pieces), high / len(pieces))
        gain = gain * jnp.repeat(jnp.exp(draws), extent[axis_at] // blocks).reshape((-1,) + (1,) * (len(extent) - 1 - axis_at))
    return gain


def profile(number_of, total, most, skew):
    portions = [(1 << 20) // math.isqrt(grade ** skew) + 1 for grade in range(2, number_of + 1)]
    surplus, counts = total - most - (number_of - 1), [1] * (number_of - 1)
    while surplus > 0:
        candidates = [i for i in range(number_of - 1) if counts[i] < most]
        mass, remaining = sum([portions[i] for i in candidates]), surplus
        for i in candidates:
            addition = min(most - counts[i], max(1, remaining * portions[i] // mass), surplus)
            counts[i] = counts[i] + addition
            surplus = surplus - addition
    return np.array([most] + counts)


def uneven_parts(rng, count, total, reach, lean):
    if count == 2:
        one = jax.random.randint(rng, (), max(1, total - reach), min(reach, total - 1) + 1)
        return jnp.stack([one, total - one])
    sizes = jnp.asarray(profile(count, total, reach, lean), jnp.int32)
    twos = (count - 1) // 2
    donor, taker = sizes[1:1 + 2 * twos:2], sizes[2:2 + 2 * twos:2]
    margin = jnp.minimum(donor - 1, reach - taker)
    moved = jax.random.randint(jax.random.fold_in(rng, 1), (twos,), 0, 1 << 20) % (margin + 1)
    sizes = sizes.at[1:1 + 2 * twos:2].set(donor - moved).at[2:2 + 2 * twos:2].set(taker + moved)
    return sizes[jax.random.permutation(jax.random.fold_in(rng, 2), count)]


def noise(own_key, shape, deviation, reach, cuts=(), kind=jnp.bfloat16):
    array = deviation * jax.random.normal(own_key, shape, jnp.float32)
    if cuts:
        array = array * level_of(own_key, shape, cuts, -0.22, 0.18)
    return jnp.clip(array, -reach, reach).astype(kind)


def setup_inputs(seed: int = 0) -> dict:
    seeds = jax.random.split(jax.random.key(seed), 28)
    return {
        "residual": noise(seeds[0], (TOKENS, D), 1.0, 6.0, ((0, 32),), jnp.float32),
        "cotangent": noise(seeds[1], (TOKENS, D), 1.0, 6.0, ((0, 32),)),
        "segments": jax.vmap(lambda own: jnp.searchsorted(jnp.cumsum(uneven_parts(own, DOCS, SEQ_LEN, DOC_MOST, 1)), jnp.arange(SEQ_LEN), side="right"))(jax.random.split(seeds[2], SEQS)).reshape((SEQS, SEQ_LEN)).astype(jnp.int32),
        "in_proj": draw_in_proj(jax.random.fold_in(seeds[27], 71), 0),
        "qv_bias": noise(seeds[4], (H, 2 * HD), 0.25, 1.5, ((0, 8), (1, 4))),
        "out_proj": noise(seeds[5], (D, D), (4 * HD) ** -0.5, 0.25, ((0, 8), (1, 4))),
        "up_proj": noise(seeds[6], (D, FF), D ** -0.5, 0.09375, ((0, 4), (1, 8))),
        "up_bias": noise(seeds[7], (FF,), 0.5, 3.0, ((0, 32),)),
        "down_proj": noise(seeds[8], (FF, D), FF ** -0.5, 0.046875, ((0, 8), (1, 4))),
        "norm_params": jnp.clip(1.0 + 0.18 * jax.random.normal(seeds[9], (4, D), jnp.float32), 0.099609375, 1.8984375).astype(jnp.bfloat16),
        "out_biases": noise(seeds[10], (2, D), 0.5, 3.0),
        "first_in_proj": noise(seeds[11], (D, H, 3 * HD), 3.0, 16.0, ((0, 4), (1, 8)), jnp.float32),
        "first_qv_bias": noise(seeds[12], (H, 2 * HD), 3.0, 16.0, ((0, 8), (1, 4)), jnp.float32),
        "first_out_proj": noise(seeds[13], (D, D), 3.0, 16.0, ((0, 8), (1, 4)), jnp.float32),
        "first_up_proj": noise(seeds[14], (D, FF), 3.0, 16.0, ((0, 4), (1, 8)), jnp.float32),
        "first_up_bias": noise(seeds[15], (FF,), 3.0, 16.0, ((0, 32),), jnp.float32),
        "first_down_proj": noise(seeds[16], (FF, D), 3.0, 16.0, ((0, 8), (1, 4)), jnp.float32),
        "first_norm_params": noise(seeds[17], (4, D), 3.0, 16.0, (), jnp.float32),
        "first_out_biases": noise(seeds[18], (2, D), 3.0, 16.0, (), jnp.float32),
        "second_in_proj": jnp.clip(jnp.exp(math.log(100.0) - 4.6051702 * jax.random.uniform(seeds[19], (D, H, 3 * HD), jnp.float32) ** level_of(seeds[19], (D, H, 3 * HD), ((0, 4), (1, 8)), -0.2, 0.2)), 1.0, 100.0),
        "second_qv_bias": jnp.clip(jnp.exp(math.log(100.0) - 4.6051702 * jax.random.uniform(seeds[20], (H, 2 * HD), jnp.float32) ** level_of(seeds[20], (H, 2 * HD), ((0, 8), (1, 4)), -0.2, 0.2)), 1.0, 100.0),
        "second_out_proj": jnp.clip(jnp.exp(math.log(100.0) - 4.6051702 * jax.random.uniform(seeds[21], (D, D), jnp.float32) ** level_of(seeds[21], (D, D), ((0, 8), (1, 4)), -0.2, 0.2)), 1.0, 100.0),
        "second_up_proj": jnp.clip(jnp.exp(math.log(100.0) - 4.6051702 * jax.random.uniform(seeds[22], (D, FF), jnp.float32) ** level_of(seeds[22], (D, FF), ((0, 4), (1, 8)), -0.2, 0.2)), 1.0, 100.0),
        "second_up_bias": jnp.clip(jnp.exp(math.log(100.0) - 4.6051702 * jax.random.uniform(seeds[23], (FF,), jnp.float32) ** level_of(seeds[23], (FF,), ((0, 32),), -0.2, 0.2)), 1.0, 100.0),
        "second_down_proj": jnp.clip(jnp.exp(math.log(100.0) - 4.6051702 * jax.random.uniform(seeds[24], (FF, D), jnp.float32) ** level_of(seeds[24], (FF, D), ((0, 8), (1, 4)), -0.2, 0.2)), 1.0, 100.0),
        "second_norm_params": jnp.clip(jnp.exp(jax.random.uniform(seeds[25], (4, D), jnp.float32, math.log(1.0), math.log(100.0))), 1.0, 100.0),
        "second_out_biases": jnp.clip(jnp.exp(jax.random.uniform(seeds[26], (2, D), jnp.float32, math.log(1.0), math.log(100.0))), 1.0, 100.0),
    }


NORM_EPS = 1e-05
BETA_FIRST = 0.9
BETA_SECOND = 0.95
ADAM_EPS = 1e-08
LEARN_RATE = 0.01
WEIGHT_DECAY = 0.1
NEG_LARGE = -1e+30

def positions_of(segments):
    index_grid = lax.broadcasted_iota(jnp.int32, segments.shape, 1)
    previous = jnp.concatenate([segments[:, :1] - 1, segments[:, :-1]], axis=1)
    starts = jnp.where(segments != previous, index_grid, 0).astype(jnp.int32)
    return (index_grid - lax.cummax(starts, axis=1)).astype(jnp.int32)

def rotation_tables(positions):
    half_rot = ROT // 2
    inv_freq = 10000.0 ** (-(2.0 * jnp.arange(half_rot, dtype=jnp.float32)) / ROT)
    angles = positions.astype(jnp.float32)[:, None] * inv_freq[None, :]
    cosine = jnp.concatenate([jnp.cos(angles), jnp.cos(angles)], axis=-1)
    sine_rows = jnp.concatenate([jnp.sin(angles), jnp.sin(angles)], axis=-1)
    return (cosine, sine_rows)

def rotate(source, cosine, sine_rows):
    half_rot = ROT // 2
    rot_part = source[..., :ROT]
    turned = jnp.concatenate([-rot_part[..., half_rot:], rot_part[..., :half_rot]], axis=-1)
    moved = rot_part * cosine[:, None, :] + turned * sine_rows[:, None, :]
    return jnp.concatenate([moved, source[..., ROT:]], axis=-1)

def normalize(source):
    centred = source - lax.optimization_barrier(jnp.mean(source, axis=-1, keepdims=True))
    inv_std = lax.rsqrt(lax.optimization_barrier(jnp.mean(centred * centred, axis=-1, keepdims=True)) + NORM_EPS)
    return (centred * inv_std, inv_std)

def gelu_slope(source):
    return 0.5 * (1.0 + lax.erf(source * (1.0 / math.sqrt(2.0)))) + source * jnp.exp(-0.5 * source * source) * (1.0 / math.sqrt(2.0 * math.pi))

def allowed_pairs(seg_row):
    length = seg_row.shape[0]
    index_grid = lax.broadcasted_iota(jnp.int32, (length, length), 0)
    column_grid = lax.broadcasted_iota(jnp.int32, (length, length), 1)
    return (column_grid <= index_grid) & (seg_row[:, None] == seg_row[None, :])

def attend(queries, key_rows, value_rows, seg_row):
    scaling = 1.0 / math.sqrt(HD)
    scores = jnp.einsum('qhd,khd->hqk', queries.astype(jnp.float32), key_rows.astype(jnp.float32)) * scaling
    scores = jnp.where(allowed_pairs(seg_row)[None], scores, NEG_LARGE)
    row_max = lax.optimization_barrier(jnp.max(scores, axis=-1, keepdims=True))
    log_total = row_max + jnp.log(lax.optimization_barrier(jnp.sum(jnp.exp(scores - row_max), axis=-1, keepdims=True)))
    attn_prob = jnp.exp(scores - log_total).astype(jnp.bfloat16)
    mixed = jnp.einsum('hqk,khd->qhd', attn_prob.astype(jnp.float32), value_rows.astype(jnp.float32))
    return (mixed.astype(jnp.bfloat16), log_total[..., 0])

def attend_back(queries, key_rows, value_rows, attended, grad_att, log_total, seg_row):
    scaling = 1.0 / math.sqrt(HD)
    scores = jnp.einsum('qhd,khd->hqk', queries.astype(jnp.float32), key_rows.astype(jnp.float32)) * scaling
    scores = jnp.where(allowed_pairs(seg_row)[None], scores, NEG_LARGE)
    prob_full = jnp.exp(scores - log_total[..., None])
    prob_round = prob_full.astype(jnp.bfloat16)
    grad_prob = jnp.einsum('qhd,khd->hqk', grad_att.astype(jnp.float32), value_rows.astype(jnp.float32))
    delta = lax.optimization_barrier(jnp.sum(grad_att.astype(jnp.float32) * attended.astype(jnp.float32), axis=-1)).T
    grad_scores = (scaling * prob_full * (grad_prob - delta[:, :, None])).astype(jnp.bfloat16)
    grad_queries = jnp.einsum('hqk,khd->qhd', grad_scores.astype(jnp.float32), key_rows.astype(jnp.float32))
    grad_keys = jnp.einsum('hqk,qhd->khd', grad_scores.astype(jnp.float32), queries.astype(jnp.float32))
    grad_values = jnp.einsum('hqk,qhd->khd', prob_round.astype(jnp.float32), grad_att.astype(jnp.float32))
    return (grad_queries, grad_keys, grad_values)

def adamw(weight, gradient, first_m, second_m, decay_rate):
    new_first = BETA_FIRST * first_m + (1.0 - BETA_FIRST) * gradient
    new_second = BETA_SECOND * second_m + (1.0 - BETA_SECOND) * gradient * gradient
    bias_one = 1.0 - BETA_FIRST ** STEP
    bias_two = 1.0 - BETA_SECOND ** STEP
    weight_f = weight.astype(jnp.float32)
    update = new_first / bias_one / (jnp.sqrt(new_second / bias_two) + ADAM_EPS) + decay_rate * weight_f
    return (gradient, weight_f - LEARN_RATE * update, new_first, new_second)

def reference(residual, cotangent, segments, in_proj, qv_bias, out_proj, up_proj, up_bias, down_proj, norm_params, out_biases, first_in_proj, first_qv_bias, first_out_proj, first_up_proj, first_up_bias, first_down_proj, first_norm_params, first_out_biases, second_in_proj, second_qv_bias, second_out_proj, second_up_proj, second_up_bias, second_down_proj, second_norm_params, second_out_biases):
    in_matrix = in_proj.reshape(D, H * 3 * HD)
    norm_f = norm_params.astype(jnp.float32)
    bias_qv = qv_bias.astype(jnp.float32)
    bias_up = up_bias.astype(jnp.float32)
    bias_out = out_biases.astype(jnp.float32)
    positions = positions_of(segments)

    def one_sequence(totals, packed):
        row_block, grad_rows, seg_row, pos_row = packed
        normed, inv_std = normalize(row_block)
        attn_in = (normed * norm_f[0] + norm_f[1]).astype(jnp.bfloat16)
        mlp_in = (normed * norm_f[2] + norm_f[3]).astype(jnp.bfloat16)
        projected = jnp.dot(attn_in, in_matrix, preferred_element_type=jnp.float32).reshape(SEQ_LEN, H, 3 * HD)
        cosine, sine_rows = rotation_tables(pos_row)
        queries = rotate(projected[:, :, :HD] + bias_qv[:, :HD], cosine, sine_rows).astype(jnp.bfloat16)
        key_rows = rotate(projected[:, :, HD:2 * HD], cosine, sine_rows).astype(jnp.bfloat16)
        value_rows = (projected[:, :, 2 * HD:] + bias_qv[:, HD:]).astype(jnp.bfloat16)
        attended, log_total = attend(queries, key_rows, value_rows, seg_row)
        flat_out = attended.reshape(SEQ_LEN, D)
        up_rows = jnp.dot(mlp_in, up_proj, preferred_element_type=jnp.float32) + bias_up
        activated = jax.nn.gelu(up_rows, approximate=False).astype(jnp.bfloat16)
        branch = jnp.dot(flat_out, out_proj, preferred_element_type=jnp.float32) + jnp.dot(activated, down_proj, preferred_element_type=jnp.float32)
        output = row_block + branch + bias_out[0] + bias_out[1]
        grad_up = jnp.dot(grad_rows, down_proj.T, preferred_element_type=jnp.float32) * gelu_slope(up_rows)
        grad_up_r = grad_up.astype(jnp.bfloat16)
        grad_down = jnp.dot(activated.T, grad_rows, preferred_element_type=jnp.float32)
        grad_upw = jnp.dot(mlp_in.T, grad_up_r, preferred_element_type=jnp.float32)
        grad_upb = lax.optimization_barrier(jnp.sum(grad_up, axis=0))
        grad_mlp_in = jnp.dot(grad_up_r, up_proj.T, preferred_element_type=jnp.float32)
        grad_flat = jnp.dot(grad_rows, out_proj.T, preferred_element_type=jnp.float32).astype(jnp.bfloat16)
        grad_outw = jnp.dot(flat_out.T, grad_rows, preferred_element_type=jnp.float32)
        grad_queries, grad_keys, grad_values = attend_back(queries, key_rows, value_rows, attended, grad_flat.reshape(SEQ_LEN, H, HD), log_total, seg_row)
        grad_queries = rotate(grad_queries, cosine, -sine_rows)
        grad_keys = rotate(grad_keys, cosine, -sine_rows)
        grad_qv = jnp.concatenate([lax.optimization_barrier(jnp.sum(grad_queries, axis=0)), lax.optimization_barrier(jnp.sum(grad_values, axis=0))], axis=-1)
        grad_projected = jnp.concatenate([grad_queries, grad_keys, grad_values], axis=-1).astype(jnp.bfloat16).reshape(SEQ_LEN, H * 3 * HD)
        grad_inw = jnp.dot(attn_in.T, grad_projected, preferred_element_type=jnp.float32)
        grad_attn_in = jnp.dot(grad_projected, in_matrix.T, preferred_element_type=jnp.float32)
        grad_norms = jnp.stack([lax.optimization_barrier(jnp.sum(grad_attn_in * normed, axis=0)), lax.optimization_barrier(jnp.sum(grad_attn_in, axis=0)), lax.optimization_barrier(jnp.sum(grad_mlp_in * normed, axis=0)), lax.optimization_barrier(jnp.sum(grad_mlp_in, axis=0))])
        column_sum = lax.optimization_barrier(jnp.sum(grad_rows.astype(jnp.float32), axis=0))
        grad_ob = jnp.stack([column_sum, column_sum])
        grad_normed = grad_attn_in * norm_f[0] + grad_mlp_in * norm_f[2]
        grad_input = grad_rows.astype(jnp.float32) + inv_std * (grad_normed - lax.optimization_barrier(jnp.mean(grad_normed, axis=-1, keepdims=True)) - normed * lax.optimization_barrier(jnp.mean(grad_normed * normed, axis=-1, keepdims=True)))
        terms = (grad_inw, grad_qv, grad_outw, grad_upw, grad_upb, grad_down, grad_norms, grad_ob)
        new_totals = tuple((total + term for total, term in zip(totals, terms)))
        return (new_totals, (output, grad_input))
    zeros = (jnp.zeros((D, H * 3 * HD), jnp.float32), jnp.zeros((H, 2 * HD), jnp.float32), jnp.zeros((D, D), jnp.float32), jnp.zeros((D, FF), jnp.float32), jnp.zeros((FF,), jnp.float32), jnp.zeros((FF, D), jnp.float32), jnp.zeros((4, D), jnp.float32), jnp.zeros((2, D), jnp.float32))
    packed = (residual.reshape(SEQS, SEQ_LEN, D), cotangent.reshape(SEQS, SEQ_LEN, D), segments, positions)
    totals, outs = lax.scan(one_sequence, zeros, packed)
    output = outs[0].reshape(TOKENS, D)
    grad_residual = outs[1].reshape(TOKENS, D)
    result_in = adamw(in_proj, totals[0].reshape(D, H, 3 * HD), first_in_proj, second_in_proj, WEIGHT_DECAY)
    result_qv = adamw(qv_bias, totals[1], first_qv_bias, second_qv_bias, 0.0)
    result_out = adamw(out_proj, totals[2], first_out_proj, second_out_proj, WEIGHT_DECAY)
    result_up = adamw(up_proj, totals[3], first_up_proj, second_up_proj, WEIGHT_DECAY)
    result_upb = adamw(up_bias, totals[4], first_up_bias, second_up_bias, 0.0)
    result_down = adamw(down_proj, totals[5], first_down_proj, second_down_proj, WEIGHT_DECAY)
    result_norm = adamw(norm_params, totals[6], first_norm_params, second_norm_params, 0.0)
    result_ob = adamw(out_biases, totals[7], first_out_biases, second_out_biases, 0.0)
    return (output, grad_residual, result_in[0], result_in[1], result_in[2], result_in[3], result_qv[0], result_qv[1], result_qv[2], result_qv[3], result_out[0], result_out[1], result_out[2], result_out[3], result_up[0], result_up[1], result_up[2], result_up[3], result_upb[0], result_upb[1], result_upb[2], result_upb[3], result_down[0], result_down[1], result_down[2], result_down[3], result_norm[0], result_norm[1], result_norm[2], result_norm[3], result_ob[0], result_ob[1], result_ob[2], result_ob[3])
```

```python
import functools
import math

import jax
import jax.numpy as jnp
from jax import lax
from jax.experimental import pallas as pl
from jax.experimental.pallas import tpu as pltpu
from jax.sharding import PartitionSpec as P


D = 4096
HD = 128
ROT = 32
SEQ_LEN = 1024
STEP = 8
DOCS = 8

NORM_EPS = 1e-05
BETA_FIRST = 0.9
BETA_SECOND = 0.95
ADAM_EPS = 1e-08
LEARN_RATE = 0.01
WEIGHT_DECAY = 0.1
NEG_LARGE = -1e30
Q_BLOCK = 256
PACK = 16

F32 = jnp.float32
BF16 = jnp.bfloat16


def positions_of(segments):
    numbers = jnp.arange(DOCS, dtype=jnp.int32)
    below = segments[:, None, :] < numbers[None, :, None]
    starts = jnp.sum(below.astype(jnp.int32), axis=-1)
    own = segments[:, :, None] == numbers[None, None, :]
    start = jnp.sum(jnp.where(own, starts[:, None, :], 0), axis=-1)
    return lax.broadcasted_iota(jnp.int32, segments.shape, 1) - start


def rotation_tables(positions):
    half_rot = ROT // 2
    inv_freq = 10000.0 ** (-(2.0 * jnp.arange(half_rot, dtype=F32)) / ROT)
    angles = positions.astype(F32)[:, None] * inv_freq[None, :]
    cosine, sine = jnp.cos(angles), jnp.sin(angles)
    rows = positions.shape[0]
    rest = HD - ROT
    ones, zeros = jnp.ones((rows, rest), F32), jnp.zeros((rows, rest), F32)
    half = jnp.zeros_like(sine)
    return (
        jnp.concatenate([cosine, cosine, ones], axis=-1),
        jnp.concatenate([-sine, half, zeros], axis=-1),
        jnp.concatenate([half, sine, zeros], axis=-1),
    )


def normalize(source):
    centred = source - jnp.mean(source, axis=-1, keepdims=True)
    inv_std = lax.rsqrt(jnp.mean(centred * centred, axis=-1, keepdims=True) + NORM_EPS)
    return centred * inv_std, inv_std


def dot_nt(left_op, right_op):
    return lax.dot_general(left_op, right_op, (((1,), (1,)), ((), ())), preferred_element_type=F32)


def dot_tn(left_op, right_op):
    return lax.dot_general(left_op, right_op, (((0,), (0,)), ((), ())), preferred_element_type=F32)


def attention_kernel(
    proj_ref, bias_ref, cos_ref, right_ref, left_ref, seg_col_ref, seg_row_ref, grad_ref,
    attended_ref, gproj_ref, gqv_ref, key_sum, value_sum,
):
    scaling = 1.0 / math.sqrt(HD)
    cosine, from_right, from_left = cos_ref[...], right_ref[...], left_ref[...]
    half_rot = ROT // 2

    def turn(source, sign):
        return source * cosine + sign * (
            pltpu.roll(source, HD - half_rot, 1) * from_right
            + pltpu.roll(source, half_rot, 1) * from_left
        )

    bias = bias_ref[0]
    queries = turn(proj_ref[:, :HD] + bias[:, :HD], 1.0).astype(BF16)
    keys = turn(proj_ref[:, HD : 2 * HD], 1.0).astype(BF16)
    values = (proj_ref[:, 2 * HD :] + bias[:, HD:]).astype(BF16)
    key_sum[...] = jnp.zeros_like(key_sum)
    value_sum[...] = jnp.zeros_like(value_sum)
    query_parts = []
    for start in range(0, SEQ_LEN, Q_BLOCK):
        rows = slice(start, start + Q_BLOCK)
        reach = start + Q_BLOCK
        query, grad = queries[rows], grad_ref[rows, :]
        key, value = keys[:reach], values[:reach]
        scores = dot_nt(query, key) * scaling
        row_at = lax.broadcasted_iota(jnp.int32, (Q_BLOCK, reach), 0) + start
        column_at = lax.broadcasted_iota(jnp.int32, (Q_BLOCK, reach), 1)
        allowed = (column_at <= row_at) & (seg_col_ref[0, rows, :] == seg_row_ref[0, :, :reach])
        scores = jnp.where(allowed, scores, NEG_LARGE)
        weights = jnp.exp(scores - jnp.max(scores, axis=-1, keepdims=True))
        prob = weights * (1.0 / jnp.sum(weights, axis=-1, keepdims=True))
        prob_round = prob.astype(BF16)
        mixed = jnp.dot(prob_round, value, preferred_element_type=F32).astype(BF16)
        attended_ref[rows, :] = mixed
        delta = jnp.sum(grad.astype(F32) * mixed.astype(F32), axis=-1, keepdims=True)
        grad_prob = dot_nt(grad, value)
        grad_scores = (scaling * prob * (grad_prob - delta)).astype(BF16)
        query_parts.append(jnp.dot(grad_scores, key, preferred_element_type=F32))
        key_sum[:reach, :] += dot_tn(grad_scores, query)
        value_sum[:reach, :] += dot_tn(prob_round, grad)
    grad_query = turn(jnp.concatenate(query_parts, axis=0), -1.0)
    grad_value = value_sum[...]
    gproj_ref[:, :HD] = grad_query.astype(BF16)
    gproj_ref[:, HD : 2 * HD] = turn(key_sum[...], -1.0).astype(BF16)
    gproj_ref[:, 2 * HD :] = grad_value.astype(BF16)
    gqv_ref[0, 0, :, :HD] = jnp.sum(grad_query, axis=0, keepdims=True)
    gqv_ref[0, 0, :, HD:] = jnp.sum(grad_value, axis=0, keepdims=True)


def attention(projected, bias_qv, tables, segments, grad_flat):
    seqs, heads = segments.shape[0], bias_qv.shape[0]
    rows = seqs * SEQ_LEN
    table = pl.BlockSpec((SEQ_LEN, HD), lambda s, h: (s, 0))
    head = pl.BlockSpec((SEQ_LEN, HD), lambda s, h: (s, h))
    packed = pl.BlockSpec((SEQ_LEN, 3 * HD), lambda s, h: (s, h))
    pairs = seqs * heads * SEQ_LEN * SEQ_LEN
    return pl.pallas_call(
        attention_kernel,
        grid=(seqs, heads),
        in_specs=[
            packed,
            pl.BlockSpec((1, 1, 2 * HD), lambda s, h: (h, 0, 0)),
            table,
            table,
            table,
            pl.BlockSpec((1, SEQ_LEN, 1), lambda s, h: (s, 0, 0)),
            pl.BlockSpec((1, 1, SEQ_LEN), lambda s, h: (s, 0, 0)),
            head,
        ],
        out_specs=[head, packed, pl.BlockSpec((1, 1, 1, 2 * HD), lambda s, h: (s, h, 0, 0))],
        out_shape=[
            jax.ShapeDtypeStruct((rows, heads * HD), BF16),
            jax.ShapeDtypeStruct((rows, heads * 3 * HD), BF16),
            jax.ShapeDtypeStruct((seqs, heads, 1, 2 * HD), F32),
        ],
        scratch_shapes=[pltpu.VMEM((SEQ_LEN, HD), F32), pltpu.VMEM((SEQ_LEN, HD), F32)],
        cost_estimate=pl.CostEstimate(
            flops=12 * pairs * HD, bytes_accessed=rows * heads * HD * 24, transcendentals=pairs
        ),
        name="attention",
    )(
        projected,
        bias_qv[:, None, :],
        *tables,
        segments[:, :, None],
        segments[:, None, :],
        grad_flat,
    )


def adamw(weight, gradient, first_m, second_m, decay_rate):
    new_first = BETA_FIRST * first_m + (1.0 - BETA_FIRST) * gradient
    new_second = BETA_SECOND * second_m + (1.0 - BETA_SECOND) * gradient * gradient
    bias_one = 1.0 - BETA_FIRST**STEP
    bias_two = 1.0 - BETA_SECOND**STEP
    weight_f = weight.astype(F32)
    update = (
        new_first / bias_one / (jnp.sqrt(new_second / bias_two) + ADAM_EPS) + decay_rate * weight_f
    )
    return (gradient, weight_f - LEARN_RATE * update, new_first, new_second)


def after(value, *others):
    return lax.optimization_barrier((value, *others))[0]


class Line:
    def __init__(self):
        self.last = None

    def __call__(self, value):
        return value if self.last is None else after(value, self.last)

    def add(self, result):
        self.last = result
        return result


def chain_gather(pieces, count):
    me = lax.axis_index("dp")
    gathered = []
    gate = None
    for piece in pieces:
        up = down = piece if gate is None else after(piece, *gate)
        ups, downs = [], []
        for hop in range(1, count):
            up = lax.ppermute(up, "dp", [(k, k + 1) for k in range(hop - 1, count - 1)])
            down = lax.ppermute(down, "dp", [(k, k - 1) for k in range(1, count - hop + 1)])
            ups.append(up)
            downs.append(down)
        gate = (ups[max(count - 3, 0)], downs[max(count - 3, 0)])
        gathered.append(
            [jnp.where(me >= h, ups[h - 1], downs[count - h - 1]) for h in range(1, count)]
        )
    return gathered


def plane_scatter(total):
    size, me = lax.axis_size("tensor"), lax.axis_index("tensor")
    bits = size.bit_length() - 1
    rows = total.shape[0] // size
    own = [(me >> bit) & 1 for bit in range(bits)]

    def step(part, left, bit):
        axis = left.index(bit)
        give = lax.dynamic_index_in_dim(part, 1 - own[bit], axis, keepdims=False)
        keep = lax.dynamic_index_in_dim(part, own[bit], axis, keepdims=False)
        got = lax.ppermute(give, "tensor", [(k, k ^ (1 << bit)) for k in range(size)])
        return keep.astype(F32) + got.astype(F32), [other for other in left if other != bit]

    left = list(range(bits))[::-1]
    part, left = step(total.reshape((2,) * bits + (rows, D)), left, 0)
    halves = []
    for at, order in enumerate((list(range(1, bits)), list(range(1, bits))[::-1])):
        half = part[..., at * (D // 2) : (at + 1) * (D // 2)]
        still = left
        for bit in order:
            half, still = step(half.astype(BF16), still, bit)
        halves.append(half)
    return jnp.concatenate(halves, axis=-1)


LANES = 128
SUBLANES = 8


def all_sum_kernel(group, x_ref, out_ref, inbox, send_one, recv_one, send_two, recv_two):
    total = group[0] * group[1]
    me = lax.axis_index("dp") * group[1] + lax.axis_index("tensor")

    def place(index):
        return {"dp": index // group[1], "tensor": index % group[1]}

    def slice_of(index):
        return pl.ds(pl.multiple_of(index * SUBLANES, SUBLANES), SUBLANES)

    def spread(step):
        peer = (me + step) % total
        return pltpu.make_async_remote_copy(
            src_ref=x_ref.at[slice_of(peer)],
            dst_ref=inbox.at[me],
            send_sem=send_one.at[step],
            recv_sem=recv_one.at[me],
            device_id=place(peer),
            device_id_type=pl.DeviceIdType.MESH,
        )

    def arrive(step):
        peer = (me + step) % total
        return pltpu.make_async_remote_copy(
            src_ref=x_ref.at[slice_of(peer)],
            dst_ref=inbox.at[peer],
            send_sem=send_one.at[step],
            recv_sem=recv_one.at[peer],
            device_id=place(peer),
            device_id_type=pl.DeviceIdType.MESH,
        )

    def hand(step):
        peer = (me + step) % total
        return pltpu.make_async_remote_copy(
            src_ref=out_ref.at[slice_of(me)],
            dst_ref=out_ref.at[slice_of(me)],
            send_sem=send_two.at[step],
            recv_sem=recv_two.at[me],
            device_id=place(peer),
            device_id_type=pl.DeviceIdType.MESH,
        )

    def take(step):
        peer = (me + step) % total
        return pltpu.make_async_remote_copy(
            src_ref=out_ref.at[slice_of(me)],
            dst_ref=out_ref.at[slice_of(peer)],
            send_sem=send_two.at[step],
            recv_sem=recv_two.at[peer],
            device_id=place(peer),
            device_id_type=pl.DeviceIdType.MESH,
        )

    barrier = pltpu.get_barrier_semaphore()

    @pl.loop(1, total)
    def _(step):
        pl.semaphore_signal(
            barrier, inc=1, device_id=place((me + step) % total),
            device_id_type=pl.DeviceIdType.MESH,
        )

    pl.semaphore_wait(barrier, total - 1)

    @pl.loop(1, total)
    def _(step):
        spread(step).start()

    @pl.loop(1, total)
    def _(step):
        arrive(step).wait_recv()

    def add(step, held):
        return held + inbox[(me + step) % total]

    out_ref[slice_of(me), :] = lax.fori_loop(1, total, add, x_ref[slice_of(me), :])

    @pl.loop(1, total)
    def _(step):
        spread(step).wait_send()

    @pl.loop(1, total)
    def _(step):
        hand(step).start()

    @pl.loop(1, total)
    def _(step):
        take(step).wait_recv()

    @pl.loop(1, total)
    def _(step):
        hand(step).wait_send()


def all_sum(values):
    group = (lax.axis_size("dp"), lax.axis_size("tensor"))
    total = group[0] * group[1]
    room = total * SUBLANES * LANES
    flat = jnp.pad(values.reshape(-1), (0, room - values.size)).reshape(-1, LANES)
    summed = pl.pallas_call(
        functools.partial(all_sum_kernel, group),
        out_shape=jax.ShapeDtypeStruct(flat.shape, F32),
        in_specs=[pl.BlockSpec(memory_space=pltpu.VMEM)],
        out_specs=pl.BlockSpec(memory_space=pltpu.VMEM),
        scratch_shapes=[pltpu.VMEM((total, SUBLANES, LANES), F32)]
        + [pltpu.SemaphoreType.DMA((total,))] * 4,
        compiler_params=pltpu.CompilerParams(collective_id=0, has_side_effects=True),
        name="all_sum",
    )(flat)
    return summed.reshape(-1)[: values.size].reshape(values.shape)


def assemble(own, others, axis):
    me = lax.axis_index("dp")
    count = len(others) + 1
    width = own.shape[axis]
    shape = list(own.shape)
    shape[axis] = width * count
    full = jnp.zeros(shape, own.dtype)
    for h, shard in enumerate([own, *others]):
        full = lax.dynamic_update_slice_in_dim(full, shard, ((me - h) % count) * width, axis)
    return full


def shards(
    residual, cotangent, segments,
    in_proj, qv_bias, out_proj, up_proj, up_bias, down_proj, norm_params, out_biases,
    first_in_proj, first_qv_bias, first_out_proj, first_up_proj, first_up_bias, first_down_proj,
    first_norm_params, first_out_biases,
    second_in_proj, second_qv_bias, second_out_proj, second_up_proj, second_up_bias,
    second_down_proj, second_norm_params, second_out_biases,
):
    count = lax.axis_size("dp")
    norm_f = norm_params.astype(F32)
    width = D // count
    heads = in_proj.shape[1]
    hidden = up_proj.shape[1]
    chunk = hidden // 2

    normed, inv_std = normalize(residual)

    in_own = in_proj.reshape(width, heads * 3 * HD)
    up_size, qv_size = up_bias.shape[0], qv_bias.size
    spare = width - up_size - qv_size

    def owner_rows(biases, projections):
        rows = jnp.concatenate([biases, projections], axis=1)
        return jnp.pad(rows, ((0, 0), (0, spare)))

    bias_row = owner_rows(up_bias[None], qv_bias.reshape(1, qv_size))
    bias_rows = jnp.pad(bias_row[:, :chunk], ((0, PACK - 1), (0, max(chunk - width, 0))))
    first_piece = jnp.concatenate([up_proj[:, :chunk], bias_rows], axis=0)
    pieces = [
        first_piece, down_proj[:chunk], up_proj[:, chunk:], down_proj[chunk:], in_own, out_proj
    ]
    others = chain_gather(pieces, count)

    group_rows = lax.all_gather(residual, "tensor", axis=0, tiled=True)
    grad_rows = lax.all_gather(cotangent, "tensor", axis=0, tiled=True)
    group_f, _ = normalize(group_rows)
    mlp_rows = (group_f * norm_f[2] + norm_f[3]).astype(BF16)
    attn_rows = (group_f * norm_f[0] + norm_f[1]).astype(BF16)
    rows_all = attn_rows.shape[0]
    tables = rotation_tables(positions_of(segments).reshape(rows_all))

    line = Line()

    def scatter(total, axis):
        return lax.psum_scatter(total, "dp", scatter_dimension=axis, tiled=True).astype(F32)

    def grow(full_up, bias):
        up_rows = jnp.dot(line(mlp_rows), full_up, preferred_element_type=F32) + bias
        normal = 0.5 * (1.0 + lax.erf(up_rows * (1.0 / math.sqrt(2.0))))
        slope = normal + up_rows * jnp.exp(-0.5 * up_rows * up_rows) * (
            1.0 / math.sqrt(2.0 * math.pi)
        )
        activated = (up_rows * normal).astype(BF16)
        line.add(activated)
        return activated, slope

    def grow_back(full_down, slope):
        grad_up = dot_nt(line(grad_rows), full_down) * slope
        grad_up_r, grad_bias = grad_up.astype(BF16), jnp.sum(grad_up, axis=0)
        line.add(grad_up_r)
        return grad_up_r, grad_bias

    def weight_grad(left_op, right_op):
        return line.add(dot_tn(line(left_op), right_op).astype(BF16))

    def product(dot, left_op, right_op, *added):
        result = dot(line(left_op), right_op)
        for more in added:
            result = result + more
        return line.add(result)

    def dot_nn(left_op, right_op):
        return jnp.dot(left_op, right_op, preferred_element_type=F32)

    shard_first = [piece[:width] for piece in others[0]]
    up_a = assemble(pieces[0][:width], shard_first, 0)
    packed = assemble(
        pieces[0][width : width + 1], [piece[width : width + 1] for piece in others[0]], 0
    )
    full_upb = packed[:, :up_size].reshape(count * up_size).astype(F32)
    full_qv = (
        packed[:, up_size : up_size + qv_size]
        .reshape(count, heads, -1)
        .transpose(1, 0, 2)
        .reshape(heads, 2 * HD)
        .astype(F32)
    )
    act_a, slope_a = grow(up_a, full_upb[:chunk])
    sdown_a = scatter(weight_grad(act_a, grad_rows), 1)
    down_a = assemble(pieces[1], others[1], 1)
    gup_a, gupb_a = grow_back(down_a, slope_a)
    sup_a = scatter(weight_grad(mlp_rows, gup_a), 0)
    grad_mlp_a = product(dot_nt, gup_a, up_a)

    up_b = assemble(pieces[2], others[2], 0)
    act_b, slope_b = grow(up_b, full_upb[chunk:])
    sdown_b = scatter(weight_grad(act_b, grad_rows), 1)
    down_b = assemble(pieces[3], others[3], 1)
    gup_b, gupb_b = grow_back(down_b, slope_b)
    sup_b = scatter(weight_grad(mlp_rows, gup_b), 0)
    grad_mlp_in = product(dot_nt, gup_b, up_b, grad_mlp_a)
    branch_mlp = product(dot_nn, act_a, down_a, dot_nn(act_b, down_b))

    full_in = assemble(pieces[4], others[4], 0)
    projected = product(dot_nn, attn_rows, full_in)
    full_out = assemble(pieces[5], others[5], 1)
    grad_flat = line.add(dot_nt(line(grad_rows), full_out).astype(BF16))
    flat_out, grad_projected, grad_qv = attention(
        projected, full_qv, tables, segments, grad_flat
    )
    line.add(grad_projected)
    grad_qv = jnp.sum(grad_qv, axis=0)[:, 0, :]
    shard_in = scatter(weight_grad(attn_rows, grad_projected), 0).reshape(width, heads, 3 * HD)

    grad_rows_of = owner_rows(
        jnp.concatenate([gupb_a, gupb_b]).reshape(count, up_size),
        grad_qv.reshape(heads, count, -1).transpose(1, 0, 2).reshape(count, qv_size),
    ).reshape(1, D)
    extra = jnp.pad(grad_rows_of.astype(BF16), ((0, PACK - 1), (0, 0)))
    grad_outw = jnp.concatenate([weight_grad(flat_out, grad_rows), extra], axis=0)
    shard_last = scatter(grad_outw, 1)
    shard_outw = shard_last[: grad_outw.shape[0] - PACK]
    shard_biases = shard_last[grad_outw.shape[0] - PACK]
    shard_upb = shard_biases[:up_size]
    shard_qv = shard_biases[up_size : up_size + qv_size].reshape(qv_bias.shape)

    branch = line.add((dot_nn(line(flat_out), full_out) + branch_mlp).astype(BF16))
    local_branch = plane_scatter(branch)
    grad_attn_in = dot_nt(line(grad_projected), full_in)
    group_grad = line.add((grad_attn_in * norm_f[0] + grad_mlp_in * norm_f[2]).astype(BF16))
    grad_norms_local = jnp.stack(
        [
            jnp.sum(grad_attn_in * group_f, axis=0),
            jnp.sum(grad_attn_in, axis=0),
            jnp.sum(grad_mlp_in * group_f, axis=0),
            jnp.sum(grad_mlp_in, axis=0),
        ]
    )
    grad_normed = plane_scatter(group_grad)
    bias_out = out_biases.astype(F32)
    output = residual + local_branch + bias_out[0] + bias_out[1]

    cotangent_f = cotangent.astype(F32)
    column_sum = jnp.sum(cotangent_f, axis=0)
    sums = all_sum(jnp.concatenate([grad_norms_local, column_sum[None]], axis=0))
    grad_norms, grad_ob = sums[:4], jnp.stack([sums[4], sums[4]])
    grad_residual = cotangent_f + inv_std * (
        grad_normed
        - jnp.mean(grad_normed, axis=-1, keepdims=True)
        - normed * jnp.mean(grad_normed * normed, axis=-1, keepdims=True)
    )
    shard_upw = jnp.concatenate([sup_a, sup_b], axis=1)
    shard_down = jnp.concatenate([sdown_a, sdown_b], axis=0)

    return (
        output,
        grad_residual,
        *adamw(in_proj, shard_in, first_in_proj, second_in_proj, WEIGHT_DECAY),
        *adamw(qv_bias, shard_qv, first_qv_bias, second_qv_bias, 0.0),
        *adamw(out_proj, shard_outw, first_out_proj, second_out_proj, WEIGHT_DECAY),
        *adamw(up_proj, shard_upw, first_up_proj, second_up_proj, WEIGHT_DECAY),
        *adamw(up_bias, shard_upb, first_up_bias, second_up_bias, 0.0),
        *adamw(down_proj, shard_down, first_down_proj, second_down_proj, WEIGHT_DECAY),
        *adamw(norm_params, grad_norms, first_norm_params, second_norm_params, 0.0),
        *adamw(out_biases, grad_ob, first_out_biases, second_out_biases, 0.0),
    )


def solution(mesh):
    rows, both = P(("dp", "tensor"), None), P(("tensor", "dp"))
    heads, in_rows, in_cols = P("dp", "tensor", None), P("dp", "tensor"), P("tensor", "dp")
    params = (heads, in_cols, in_cols, in_rows, both, in_cols, P(), P())
    in_specs = (rows, rows, P("dp", None)) + params * 3
    out_specs = (rows, rows) + tuple(spec for spec in params for _ in range(4))

    return jax.shard_map(shards, mesh=mesh, in_specs=in_specs, out_specs=out_specs, check_vma=False)
```

```python
import functools
import math

import jax
import jax.numpy as jnp
from jax import lax
from jax.experimental import pallas as pl
from jax.experimental.pallas import tpu as pltpu
from jax.experimental.layout import Layout, with_layout_constraint
from jax.sharding import PartitionSpec as P


D = 4096
HD = 128
ROT = 32
SEQ_LEN = 1024
STEP = 8
DOCS = 8

NORM_EPS = 1e-05
BETA_FIRST = 0.9
BETA_SECOND = 0.95
ADAM_EPS = 1e-08
LEARN_RATE = 0.01
WEIGHT_DECAY = 0.1
NEG_LARGE = -1e30
Q_BLOCK = 256
PACK = 16
GROUPS = 2
DP, TENSOR = "dp", "tensor"


F32 = jnp.float32
BF16 = jnp.bfloat16


def positions_of(segments):
    numbers = jnp.arange(DOCS, dtype=jnp.int32)
    below = segments[:, None, :] < numbers[None, :, None]
    starts = jnp.sum(below.astype(jnp.int32), axis=-1)
    own = segments[:, :, None] == numbers[None, None, :]
    start = jnp.sum(jnp.where(own, starts[:, None, :], 0), axis=-1)
    return lax.broadcasted_iota(jnp.int32, segments.shape, 1) - start


def rotation_tables(positions):
    half_rot = ROT // 2
    inv_freq = 10000.0 ** (-(2.0 * jnp.arange(half_rot, dtype=F32)) / ROT)
    angles = positions.astype(F32)[:, None] * inv_freq[None, :]
    cosine, sine = jnp.cos(angles), jnp.sin(angles)
    rows = positions.shape[0]
    rest = HD - ROT
    ones, zeros = jnp.ones((rows, rest), F32), jnp.zeros((rows, rest), F32)
    half = jnp.zeros_like(sine)
    return (
        jnp.concatenate([cosine, cosine, ones], axis=-1),
        jnp.concatenate([-sine, half, zeros], axis=-1),
        jnp.concatenate([half, sine, zeros], axis=-1),
    )


def normalize(source):
    centred = source - jnp.mean(source, axis=-1, keepdims=True)
    inv_std = lax.rsqrt(jnp.mean(centred * centred, axis=-1, keepdims=True) + NORM_EPS)
    return centred * inv_std, inv_std


def dot_nt(left_op, right_op):
    return lax.dot_general(left_op, right_op, (((1,), (1,)), ((), ())), preferred_element_type=F32)


def dot_tn(left_op, right_op):
    return lax.dot_general(left_op, right_op, (((0,), (0,)), ((), ())), preferred_element_type=F32)


def attention_kernel(
    proj_ref, bias_ref, cos_ref, right_ref, left_ref, seg_col_ref, seg_row_ref, grad_ref,
    attended_ref, gproj_ref, gqv_ref, key_sum, value_sum,
):
    scaling = 1.0 / math.sqrt(HD)
    cosine, from_right, from_left = cos_ref[...], right_ref[...], left_ref[...]
    half_rot = ROT // 2

    def turn(source, sign):
        return source * cosine + sign * (
            pltpu.roll(source, HD - half_rot, 1) * from_right
            + pltpu.roll(source, half_rot, 1) * from_left
        )

    bias = bias_ref[0]
    queries = turn(proj_ref[:, :HD] + bias[:, :HD], 1.0).astype(BF16)
    keys = turn(proj_ref[:, HD : 2 * HD], 1.0).astype(BF16)
    values = (proj_ref[:, 2 * HD :] + bias[:, HD:]).astype(BF16)
    key_sum[...] = jnp.zeros_like(key_sum)
    value_sum[...] = jnp.zeros_like(value_sum)
    query_parts = []
    for start in range(0, SEQ_LEN, Q_BLOCK):
        rows = slice(start, start + Q_BLOCK)
        reach = start + Q_BLOCK
        query, grad = queries[rows], grad_ref[rows, :]
        key, value = keys[:reach], values[:reach]
        scores = dot_nt(query, key) * scaling
        row_at = lax.broadcasted_iota(jnp.int32, (Q_BLOCK, reach), 0) + start
        column_at = lax.broadcasted_iota(jnp.int32, (Q_BLOCK, reach), 1)
        allowed = (column_at <= row_at) & (seg_col_ref[0, rows, :] == seg_row_ref[0, :, :reach])
        scores = jnp.where(allowed, scores, NEG_LARGE)
        weights = jnp.exp(scores - jnp.max(scores, axis=-1, keepdims=True))
        prob = weights * (1.0 / jnp.sum(weights, axis=-1, keepdims=True))
        prob_round = prob.astype(BF16)
        mixed = jnp.dot(prob_round, value, preferred_element_type=F32).astype(BF16)
        attended_ref[rows, :] = mixed
        delta = jnp.sum(grad.astype(F32) * mixed.astype(F32), axis=-1, keepdims=True)
        grad_prob = dot_nt(grad, value)
        grad_scores = (scaling * prob * (grad_prob - delta)).astype(BF16)
        query_parts.append(jnp.dot(grad_scores, key, preferred_element_type=F32))
        key_sum[:reach, :] += dot_tn(grad_scores, query)
        value_sum[:reach, :] += dot_tn(prob_round, grad)
    grad_query = turn(jnp.concatenate(query_parts, axis=0), -1.0)
    grad_value = value_sum[...]
    gproj_ref[:, :HD] = grad_query.astype(BF16)
    gproj_ref[:, HD : 2 * HD] = turn(key_sum[...], -1.0).astype(BF16)
    gproj_ref[:, 2 * HD :] = grad_value.astype(BF16)
    gqv_ref[0, 0, :, :HD] = jnp.sum(grad_query, axis=0, keepdims=True)
    gqv_ref[0, 0, :, HD:] = jnp.sum(grad_value, axis=0, keepdims=True)


def attention(projected, bias_qv, tables, segments, grad_flat):
    seqs, heads = segments.shape[0], bias_qv.shape[0]
    rows = seqs * SEQ_LEN
    table = pl.BlockSpec((SEQ_LEN, HD), lambda s, h: (s, 0))
    head = pl.BlockSpec((SEQ_LEN, HD), lambda s, h: (s, h))
    packed = pl.BlockSpec((SEQ_LEN, 3 * HD), lambda s, h: (s, h))
    pairs = seqs * heads * SEQ_LEN * SEQ_LEN
    return pl.pallas_call(
        attention_kernel,
        grid=(seqs, heads),
        in_specs=[
            packed,
            pl.BlockSpec((1, 1, 2 * HD), lambda s, h: (h, 0, 0)),
            table,
            table,
            table,
            pl.BlockSpec((1, SEQ_LEN, 1), lambda s, h: (s, 0, 0)),
            pl.BlockSpec((1, 1, SEQ_LEN), lambda s, h: (s, 0, 0)),
            head,
        ],
        out_specs=[head, packed, pl.BlockSpec((1, 1, 1, 2 * HD), lambda s, h: (s, h, 0, 0))],
        out_shape=[
            jax.ShapeDtypeStruct((rows, heads * HD), BF16),
            jax.ShapeDtypeStruct((rows, heads * 3 * HD), BF16),
            jax.ShapeDtypeStruct((seqs, heads, 1, 2 * HD), F32),
        ],
        scratch_shapes=[pltpu.VMEM((SEQ_LEN, HD), F32), pltpu.VMEM((SEQ_LEN, HD), F32)],
        cost_estimate=pl.CostEstimate(
            flops=12 * pairs * HD, bytes_accessed=rows * heads * HD * 24, transcendentals=pairs
        ),
        name="attention",
    )(
        projected,
        bias_qv[:, None, :],
        *tables,
        segments[:, :, None],
        segments[:, None, :],
        grad_flat,
    )


def adamw(weight, gradient, first_m, second_m, decay_rate):
    new_first = BETA_FIRST * first_m + (1.0 - BETA_FIRST) * gradient
    new_second = BETA_SECOND * second_m + (1.0 - BETA_SECOND) * gradient * gradient
    bias_one = 1.0 - BETA_FIRST**STEP
    bias_two = 1.0 - BETA_SECOND**STEP
    weight_f = weight.astype(F32)
    update = (
        new_first / bias_one / (jnp.sqrt(new_second / bias_two) + ADAM_EPS) + decay_rate * weight_f
    )
    return (gradient, weight_f - LEARN_RATE * update, new_first, new_second)


def by_rows(value):
    return with_layout_constraint(value, Layout(major_to_minor=(0, 1)))


def after(value, *others):
    return lax.optimization_barrier((value, *others))[0]


class Line:
    def __init__(self):
        self.last = None

    def __call__(self, value):
        return value if self.last is None else after(value, self.last)

    def add(self, result):
        self.last = result
        return result


def chain_gather(pieces, count):
    me = lax.axis_index(DP)
    gathered = []
    gate = None
    for piece in pieces:
        up = down = piece if gate is None else after(piece, *gate)
        ups, downs = [], []
        for hop in range(1, count - 1):
            up = lax.ppermute(up, DP, [(k, k + 1) for k in range(hop - 1, count - 1)])
            down = lax.ppermute(down, DP, [(k, k - 1) for k in range(1, count - hop + 1)])
            ups.append(up)
            downs.append(down)
        gate = (ups[max(count - 3, 0)], downs[max(count - 3, 0)])
        inner = lax.optimization_barrier(jnp.where(2 * me >= count, up, down))
        ends = lax.ppermute(inner, DP, [(count - 2, count - 1), (1, 0)])
        ups.append(ends)
        downs.append(ends)
        choices = [(ups[h - 1], downs[count - h - 1]) for h in range(1, count)]
        if count == 4:
            choices[1] = (inner, inner)
        gathered.append(choices)
    return gathered


def chosen(choices, wait):
    me = lax.axis_index(DP)
    return [
        wait(up) if up is down else jnp.where(me >= h, wait(up), wait(down))
        for h, (up, down) in enumerate(choices, 1)
    ]


def chain_scatter(block_of, count):
    me = lax.axis_index(DP)
    first = lax.ppermute(
        block_of(jnp.where(2 * me < count, count - 1, 0)),
        DP,
        [(0, 1), (count - 1, count - 2)],
    )
    held = (first, first)
    for hop in range(2, count):
        pairs = [(k, k + 1) for k in range(hop)]
        mirrored = [(count - 1 - here, count - 1 - there) for here, there in pairs]
        sent = []
        for owner, partial in zip((me + count - hop, me - count + hop), held):
            block = block_of(jnp.clip(owner, 0, count - 1))
            sent.append((block.astype(F32) + partial.astype(F32)).astype(BF16))
        held = lax.optimization_barrier(
            (lax.ppermute(sent[0], DP, pairs), lax.ppermute(sent[1], DP, mirrored))
        )
    return block_of(me).astype(F32) + held[0].astype(F32) + held[1].astype(F32)


LANES = 128
SUBLANES = 8


def all_sum_kernel(group, x_ref, out_ref, inbox, send_one, recv_one, send_two, recv_two):
    total = group[0] * group[1]
    me = lax.axis_index(DP) * group[1] + lax.axis_index(TENSOR)

    def place(index):
        return {DP: index // group[1], TENSOR: index % group[1]}

    def slice_of(index):
        return pl.ds(pl.multiple_of(index * SUBLANES, SUBLANES), SUBLANES)

    def spread(step):
        peer = (me + step) % total
        return pltpu.make_async_remote_copy(
            src_ref=x_ref.at[slice_of(peer)],
            dst_ref=inbox.at[me],
            send_sem=send_one.at[step],
            recv_sem=recv_one.at[me],
            device_id=place(peer),
            device_id_type=pl.DeviceIdType.MESH,
        )

    def arrive(step):
        peer = (me + step) % total
        return pltpu.make_async_remote_copy(
            src_ref=x_ref.at[slice_of(peer)],
            dst_ref=inbox.at[peer],
            send_sem=send_one.at[step],
            recv_sem=recv_one.at[peer],
            device_id=place(peer),
            device_id_type=pl.DeviceIdType.MESH,
        )

    def hand(step):
        peer = (me + step) % total
        return pltpu.make_async_remote_copy(
            src_ref=out_ref.at[slice_of(me)],
            dst_ref=out_ref.at[slice_of(me)],
            send_sem=send_two.at[step],
            recv_sem=recv_two.at[me],
            device_id=place(peer),
            device_id_type=pl.DeviceIdType.MESH,
        )

    def take(step):
        peer = (me + step) % total
        return pltpu.make_async_remote_copy(
            src_ref=out_ref.at[slice_of(me)],
            dst_ref=out_ref.at[slice_of(peer)],
            send_sem=send_two.at[step],
            recv_sem=recv_two.at[peer],
            device_id=place(peer),
            device_id_type=pl.DeviceIdType.MESH,
        )

    barrier = pltpu.get_barrier_semaphore()

    @pl.loop(1, total)
    def _(step):
        pl.semaphore_signal(
            barrier, inc=1, device_id=place((me + step) % total),
            device_id_type=pl.DeviceIdType.MESH,
        )

    pl.semaphore_wait(barrier, total - 1)

    @pl.loop(1, total)
    def _(step):
        spread(step).start()

    @pl.loop(1, total)
    def _(step):
        arrive(step).wait_recv()

    def add(step, held):
        return held + inbox[(me + step) % total]

    out_ref[slice_of(me), :] = lax.fori_loop(1, total, add, x_ref[slice_of(me), :])

    @pl.loop(1, total)
    def _(step):
        spread(step).wait_send()

    @pl.loop(1, total)
    def _(step):
        hand(step).start()

    @pl.loop(1, total)
    def _(step):
        take(step).wait_recv()

    @pl.loop(1, total)
    def _(step):
        hand(step).wait_send()


def all_sum(values):
    group = (lax.axis_size(DP), lax.axis_size(TENSOR))
    total = group[0] * group[1]
    room = total * SUBLANES * LANES
    flat = jnp.pad(values.reshape(-1), (0, room - values.size)).reshape(-1, LANES)
    summed = pl.pallas_call(
        functools.partial(all_sum_kernel, group),
        out_shape=jax.ShapeDtypeStruct(flat.shape, F32),
        in_specs=[pl.BlockSpec(memory_space=pltpu.VMEM)],
        out_specs=pl.BlockSpec(memory_space=pltpu.VMEM),
        scratch_shapes=[pltpu.VMEM((total, SUBLANES, LANES), F32)]
        + [pltpu.SemaphoreType.DMA((total,))] * 4,
        compiler_params=pltpu.CompilerParams(collective_id=0, has_side_effects=True),
    )(flat)
    return summed.reshape(-1)[: values.size].reshape(values.shape)


def assemble(own, others, axis):
    me = lax.axis_index(DP)
    count = len(others) + 1
    width = own.shape[axis]
    shape = list(own.shape)
    shape[axis] = width * count
    full = jnp.zeros(shape, own.dtype)
    for h, shard in enumerate([own, *others]):
        full = lax.dynamic_update_slice_in_dim(full, shard, ((me - h) % count) * width, axis)
    return full


def shards(
    residual, cotangent, segments,
    in_proj, qv_bias, out_proj, up_proj, up_bias, down_proj, norm_params, out_biases,
    first_in_proj, first_qv_bias, first_out_proj, first_up_proj, first_up_bias, first_down_proj,
    first_norm_params, first_out_biases,
    second_in_proj, second_qv_bias, second_out_proj, second_up_proj, second_up_bias,
    second_down_proj, second_norm_params, second_out_biases,
):
    count = lax.axis_size(DP)
    norm_f = norm_params.astype(F32)
    width = D // count
    heads = in_proj.shape[1]
    hidden = up_proj.shape[1]
    chunk = hidden // 2

    normed, inv_std = normalize(residual)

    in_own = in_proj.reshape(width, heads * 3 * HD)
    up_size, qv_size = up_bias.shape[0], qv_bias.size
    spare = width - up_size - qv_size

    def owner_rows(biases, projections):
        rows = jnp.concatenate([biases, projections], axis=1)
        return jnp.pad(rows, ((0, 0), (0, spare)))

    bias_row = owner_rows(up_bias[None], qv_bias.reshape(1, qv_size))
    bias_rows = jnp.pad(bias_row[:, :chunk], ((0, PACK - 1), (0, max(chunk - width, 0))))
    first_piece = jnp.concatenate([up_proj[:, :chunk], bias_rows], axis=0)
    part = heads * 3 * HD // GROUPS
    tile = heads * HD // GROUPS

    def pack(in_part, out_part):
        stacked = [out_part[:, at : at + tile] for at in range(0, width, tile)]
        return jnp.concatenate([in_part, jnp.concatenate(stacked, axis=0)], axis=1)

    def unpack(packed):
        rows = [packed[at : at + tile, part:] for at in range(0, width, tile)]
        return packed[:width, :part], jnp.concatenate(rows, axis=1)

    in_parts = [in_own[:, at * part : (at + 1) * part] for at in range(GROUPS)]
    out_parts = [out_proj[at * tile : (at + 1) * tile] for at in range(GROUPS)]
    pieces = [
        first_piece, down_proj[:chunk], up_proj[:, chunk:], down_proj[chunk:],
        *(pack(*parts) for parts in zip(in_parts, out_parts)),
    ]
    others = chain_gather(pieces, count)

    group_rows = lax.all_gather(residual, TENSOR, axis=0, tiled=True)
    grad_rows = lax.all_gather(cotangent, TENSOR, axis=0, tiled=True)
    group_f, _ = normalize(group_rows)
    mlp_rows = (group_f * norm_f[2] + norm_f[3]).astype(BF16)
    attn_rows = (group_f * norm_f[0] + norm_f[1]).astype(BF16)
    rows_all = attn_rows.shape[0]
    tables = rotation_tables(positions_of(segments).reshape(rows_all))

    line = Line()
    line.add(mlp_rows)

    def scatter(total, axis):
        def block_of(owner):
            return lax.dynamic_slice_in_dim(total, owner * width, width, axis)

        return chain_scatter(block_of, count)

    def plane_scatter(total):
        return lax.psum_scatter(total, TENSOR, scatter_dimension=0, tiled=True).astype(F32)

    def grow(full_up, bias):
        up_rows = jnp.dot(line(mlp_rows), full_up, preferred_element_type=F32) + bias
        normal = 0.5 * (1.0 + lax.erf(up_rows * (1.0 / math.sqrt(2.0))))
        slope = normal + up_rows * jnp.exp(-0.5 * up_rows * up_rows) * (
            1.0 / math.sqrt(2.0 * math.pi)
        )
        activated = (up_rows * normal).astype(BF16)
        line.add(activated)
        return activated, slope

    def grow_back(full_down, slope):
        grad_up = dot_nt(line(grad_rows), full_down) * slope
        grad_up_r, grad_bias = grad_up.astype(BF16), jnp.sum(grad_up, axis=0)
        line.add(grad_up_r)
        return grad_up_r, grad_bias

    def weight_grad(left_op, right_op):
        return line.add(dot_tn(line(left_op), right_op).astype(BF16))

    def product(dot, left_op, right_op, *added):
        return line.add(sum(added, dot(line(left_op), right_op)))

    def dot_nn(left_op, right_op):
        return jnp.dot(left_op, right_op, preferred_element_type=F32)

    first_others = chosen(others[0], line)
    shard_first = [piece[:width] for piece in first_others]
    up_a = assemble(pieces[0][:width], shard_first, 0)
    packed = assemble(
        pieces[0][width : width + 1], [piece[width : width + 1] for piece in first_others], 0
    )
    full_upb = packed[:, :up_size].reshape(count * up_size).astype(F32)
    full_qv = (
        packed[:, up_size : up_size + qv_size]
        .reshape(count, heads, -1)
        .transpose(1, 0, 2)
        .reshape(heads, 2 * HD)
        .astype(F32)
    )
    act_a, slope_a = grow(up_a, full_upb[:chunk])
    sdown_a = scatter(weight_grad(act_a, grad_rows), 1)
    down_a = assemble(pieces[1], chosen(others[1], line), 1)
    gup_a, gupb_a = grow_back(down_a, slope_a)
    sup_a = scatter(weight_grad(mlp_rows, gup_a), 0)
    mlp_in_a = product(dot_nt, gup_a, up_a)

    up_b = assemble(pieces[2], chosen(others[2], line), 0)
    act_b, slope_b = grow(up_b, full_upb[chunk:])
    sdown_b = scatter(weight_grad(act_b, grad_rows), 1)
    branch_a = product(dot_nn, act_a, down_a)
    down_b = assemble(pieces[3], chosen(others[3], line), 1)
    gup_b, gupb_b = grow_back(down_b, slope_b)
    sup_b = scatter(weight_grad(mlp_rows, gup_b), 0)
    grad_mlp_in = product(dot_nt, gup_b, up_b, mlp_in_a)
    branch_mlp = product(dot_nn, act_b, down_b, branch_a)

    group = heads // GROUPS
    full_ins, full_outs, flat_outs, grad_projs, grad_qvs, shard_groups = [], [], [], [], [], []
    for at in range(GROUPS):
        received = [unpack(piece) for piece in chosen(others[4 + at], line)]
        full_in = assemble(in_parts[at], [piece[0] for piece in received], 0)
        full_out = assemble(out_parts[at], [piece[1] for piece in received], 1)
        projected = product(dot_nn, attn_rows, full_in)
        grad_flat = line.add(dot_nt(line(grad_rows), full_out).astype(BF16))
        flat_out, grad_projected, grad_qv = attention(
            projected, full_qv[at * group : (at + 1) * group], tables, segments, grad_flat
        )
        line.add(grad_projected)
        full_ins.append(full_in)
        full_outs.append(full_out)
        flat_outs.append(flat_out)
        grad_projs.append(grad_projected)
        grad_qvs.append(jnp.sum(grad_qv, axis=0)[:, 0, :])
        final = at == GROUPS - 1
        if final:
            mixed = dot_nn(
                line(jnp.concatenate(flat_outs, axis=1)), jnp.concatenate(full_outs, axis=0)
            )
            branch = line.add((mixed + branch_mlp).astype(BF16))
            local_branch = plane_scatter(branch)
            bias_rows_of = owner_rows(
                jnp.concatenate([gupb_a, gupb_b]).reshape(count, up_size),
                jnp.concatenate(grad_qvs, axis=0)
                .reshape(heads, count, -1)
                .transpose(1, 0, 2)
                .reshape(count, qv_size),
            ).astype(BF16)
        grad_inw = weight_grad(attn_rows, grad_projected)
        grad_outw = weight_grad(flat_out, grad_rows)

        def owner_block(owner, grad_inw=grad_inw, grad_outw=grad_outw, final=final):
            block = pack(
                lax.dynamic_slice_in_dim(grad_inw, owner * width, width, 0),
                lax.dynamic_slice_in_dim(grad_outw, owner * width, width, 1),
            )
            if not final:
                return block
            row = lax.dynamic_slice_in_dim(bias_rows_of, owner, 1, 0)
            return jnp.concatenate([block, jnp.pad(row, ((0, PACK - 1), (0, 0)))], axis=0)

        shard_groups.append(chain_scatter(owner_block, count))
    unpacked = [unpack(shard) for shard in shard_groups]
    shard_in = jnp.concatenate(
        [shard.reshape(width, group, 3 * HD) for shard, _ in unpacked], axis=1
    )
    shard_outw = by_rows(jnp.concatenate([shard for _, shard in unpacked], axis=0))
    shard_upb = shard_groups[-1][width, :up_size]
    shard_qv = shard_groups[-1][width, up_size : up_size + qv_size].reshape(qv_bias.shape)

    grad_attn_in = dot_nt(
        line(jnp.concatenate(grad_projs, axis=1)), jnp.concatenate(full_ins, axis=1)
    )
    group_grad = line.add((grad_attn_in * norm_f[0] + grad_mlp_in * norm_f[2]).astype(BF16))
    grad_norms_local = jnp.stack(
        [
            jnp.sum(grad_attn_in * group_f, axis=0),
            jnp.sum(grad_attn_in, axis=0),
            jnp.sum(grad_mlp_in * group_f, axis=0),
            jnp.sum(grad_mlp_in, axis=0),
        ]
    )
    grad_normed = plane_scatter(group_grad)
    bias_out = out_biases.astype(F32)
    output = residual + local_branch + bias_out[0] + bias_out[1]

    column_sum = jnp.sum(cotangent.astype(F32), axis=0)
    cotangent_f = after(cotangent, column_sum).astype(F32)
    local_sums = jnp.concatenate([grad_norms_local, column_sum[None]], axis=0)
    sums = all_sum(after(local_sums, shard_upb))
    grad_norms, grad_ob = sums[:4], jnp.stack([sums[4], sums[4]])
    grad_residual = cotangent_f + inv_std * (
        grad_normed
        - jnp.mean(grad_normed, axis=-1, keepdims=True)
        - normed * jnp.mean(grad_normed * normed, axis=-1, keepdims=True)
    )
    shard_upw = jnp.concatenate([by_rows(sup_a), by_rows(sup_b)], axis=1)
    shard_down = jnp.concatenate([sdown_a, sdown_b], axis=0)
    result_in = adamw(in_proj, shard_in, first_in_proj, second_in_proj, WEIGHT_DECAY)
    result_out = adamw(out_proj, shard_outw, first_out_proj, second_out_proj, WEIGHT_DECAY)
    result_up = adamw(up_proj, shard_upw, first_up_proj, second_up_proj, WEIGHT_DECAY)
    result_down = adamw(
        down_proj, shard_down, first_down_proj, second_down_proj, WEIGHT_DECAY
    )

    return (
        output,
        grad_residual,
        *result_in,
        *adamw(qv_bias, shard_qv, first_qv_bias, second_qv_bias, 0.0),
        *result_out,
        *result_up,
        *adamw(up_bias, shard_upb, first_up_bias, second_up_bias, 0.0),
        *result_down,
        *adamw(norm_params, grad_norms, first_norm_params, second_norm_params, 0.0),
        *adamw(out_biases, grad_ob, first_out_biases, second_out_biases, 0.0),
    )


def solution(mesh):
    rows, both = P((DP, TENSOR), None), P((TENSOR, DP))
    heads, in_rows, in_cols = P(DP, TENSOR, None), P(DP, TENSOR), P(TENSOR, DP)
    params = (heads, in_cols, in_cols, in_rows, both, in_cols, P(), P())
    in_specs = (rows, rows, P(DP, None)) + params * 3
    out_specs = (rows, rows) + tuple(spec for spec in params for _ in range(4))

    return jax.shard_map(shards, mesh=mesh, in_specs=in_specs, out_specs=out_specs, check_vma=False)
```
